32 devices in a mesh: dp: 4 (over y, z), sp: 8 (over x, core).
Axes of the slice: x: 4, y: 2, z: 2, core: 2. Of those that a mesh axis runs over, the one named last changes fastest.
The devices are a block of a 4x4x8 slice.
Arguments:
- resid_x: bfloat16 [64, 1024, 2048], P('dp', 'sp'), parts along dimension 0
- positions: int32 [64, 1024], P('dp', 'sp'), parts along dimension 0
- w_query: bfloat16 [2048, 2048], replicated
- w_key: bfloat16 [2048, 2048], replicated
- w_value: bfloat16 [2048, 2048], replicated
- w_out: bfloat16 [2048, 2048], replicated
- gain_q: bfloat16 [2048], replicated
- gain_k: bfloat16 [2048], replicated
- gain_out: bfloat16 [2048], replicated
Outputs:
- output: bfloat16 [64, 1024, 2048], P('dp', 'sp'), parts along dimension 0
There are 4 independent parts. The reference program is written for one: setup_inputs(seed, part) draws one part's arguments, and reference() takes and returns one part's arrays. A program takes and returns all parts, laid end to end along the dimension named above; an argument that names none is the same for every part.
All inputs are finite; a program needn't handle non-finite values.
Results may differ from the reference program's by a relative error of at most 0.0179203.
Values are sent between devices in bfloat16 or wider.
A program may use at most 768 MiB of HBM per device.

```python
import jax
import jax.numpy as jnp
from jax import lax

BATCH = 16
SEQ = 1024
D_MODEL = 2048
HEADS = 16
HEAD_DIM = 128
DOC_LEN = 512
QUERY_BLOCKS = 8
ROPE_THETA = 500000.0
NORM_EPS = 1e-6
SCALE = HEAD_DIM ** -0.5


def setup_inputs(seed: int = 0, part: int = 0) -> dict:
    base_key = jax.random.key(seed)
    shared_keys = jax.random.split(base_key, 8)
    part_keys = jax.random.split(jax.random.fold_in(shared_keys[7], part), 2)
    resid_x = jax.random.normal(part_keys[0], (BATCH, SEQ, D_MODEL), jnp.float32).astype(jnp.bfloat16)
    token_idx = jnp.arange(SEQ, dtype=jnp.int32)[None, :]
    starts = jax.random.randint(part_keys[1], (BATCH, SEQ), 0, DOC_LEN) == 0
    starts = jnp.logical_or(starts, token_idx == 0)
    last_start = lax.cummax(jnp.where(starts, token_idx, 0), axis=1)
    positions = (token_idx - last_start).astype(jnp.int32)
    w_scale = D_MODEL ** -0.5
    matrices = [(jax.random.normal(shared_keys[w_idx], (D_MODEL, D_MODEL), jnp.float32) * w_scale).astype(jnp.bfloat16) for w_idx in range(4)]
    gains = [(0.5 + jax.random.normal(shared_keys[4 + g_idx], (D_MODEL,), jnp.float32)).astype(jnp.bfloat16) for g_idx in range(3)]
    return {'resid_x': resid_x, 'positions': positions, 'w_query': matrices[0], 'w_key': matrices[1], 'w_value': matrices[2], 'w_out': matrices[3], 'gain_q': gains[0], 'gain_k': gains[1], 'gain_out': gains[2]}


def rope_tables(pos_ids):
    inv_freq = 1.0 / (ROPE_THETA ** (jnp.arange(0, HEAD_DIM, 2, dtype=jnp.float32) / HEAD_DIM))
    angles = pos_ids.astype(jnp.float32)[..., None] * inv_freq
    return jnp.cos(angles), jnp.sin(angles)


def apply_rope(heads_f32, cos_t, sin_t):
    half = HEAD_DIM // 2
    cos_b = cos_t[:, :, None, :]
    sin_b = sin_t[:, :, None, :]
    first = heads_f32[..., :half]
    second = heads_f32[..., half:]
    return jnp.concatenate([first * cos_b - second * sin_b, second * cos_b + first * sin_b], axis=-1)


def rms_scale(vals_f32, gain):
    mean_sq = jnp.mean(vals_f32 * vals_f32, axis=-1, keepdims=True)
    return vals_f32 * lax.rsqrt(mean_sq + NORM_EPS) * gain.astype(jnp.float32)


def norm_rope(x_rows, weight, gain, cos_t, sin_t):
    proj = jnp.dot(x_rows, weight, preferred_element_type=jnp.float32).astype(jnp.bfloat16).astype(jnp.float32)
    normed = rms_scale(proj, gain).reshape(BATCH, SEQ, HEADS, HEAD_DIM)
    return apply_rope(normed, cos_t, sin_t).astype(jnp.bfloat16)


def head_attention(operands):
    q_head, k_head, v_head = operands
    block = SEQ // QUERY_BLOCKS
    q_blocks = q_head.reshape(BATCH, QUERY_BLOCKS, block, HEAD_DIM).transpose(1, 0, 2, 3)
    k_f32 = k_head.astype(jnp.float32)
    v_f32 = v_head.astype(jnp.float32)
    key_idx = jnp.arange(SEQ)

    def one_block(blk_ops):
        q_blk, blk_idx = blk_ops
        scores = jnp.einsum('bqd,bkd->bqk', q_blk.astype(jnp.float32), k_f32) * SCALE
        q_idx = blk_idx * block + jnp.arange(block)
        mask = key_idx[None, :] <= q_idx[:, None]
        scores = jnp.where(mask[None], scores, -1e30)
        probs = jax.nn.softmax(scores, axis=-1).astype(jnp.bfloat16).astype(jnp.float32)
        return jnp.einsum('bqk,bkd->bqd', probs, v_f32).astype(jnp.bfloat16)

    out_blocks = lax.map(one_block, (q_blocks, jnp.arange(QUERY_BLOCKS)))
    return out_blocks.transpose(1, 0, 2, 3).reshape(BATCH, SEQ, HEAD_DIM)


def reference(resid_x, positions, w_query, w_key, w_value, w_out, gain_q, gain_k, gain_out):
    cos_t, sin_t = rope_tables(positions)
    x_rows = resid_x.reshape(BATCH * SEQ, D_MODEL)
    q_all = norm_rope(x_rows, w_query, gain_q, cos_t, sin_t)
    k_all = norm_rope(x_rows, w_key, gain_k, cos_t, sin_t)
    v_all = jnp.dot(x_rows, w_value, preferred_element_type=jnp.float32).astype(jnp.bfloat16).reshape(BATCH, SEQ, HEADS, HEAD_DIM)
    per_head = lax.map(head_attention, (q_all.transpose(2, 0, 1, 3), k_all.transpose(2, 0, 1, 3), v_all.transpose(2, 0, 1, 3)))
    attn_rows = per_head.transpose(1, 2, 0, 3).reshape(BATCH * SEQ, D_MODEL)
    attn_out = jnp.dot(attn_rows, w_out, preferred_element_type=jnp.float32).astype(jnp.bfloat16).astype(jnp.float32)
    y_rows = x_rows.astype(jnp.float32) + rms_scale(attn_out, gain_out)
    return y_rows.astype(jnp.bfloat16).reshape(BATCH, SEQ, D_MODEL)
```

```python
import functools

import numpy as np
import jax
import jax.numpy as jnp
from jax import lax
from jax.experimental import pallas as pl
from jax.experimental.pallas import tpu as pltpu
from jax.sharding import PartitionSpec as P

HEAD_DIM = 128
HALF = HEAD_DIM // 2
ROPE_THETA = 500000.0
NORM_EPS = 1e-6
SCALE = HEAD_DIM ** -0.5
EXP2_SCALE = SCALE * 1.4426950408889634
NEG = -1e30
TN = 512
F32 = jnp.float32
BF16 = jnp.bfloat16


def kernel(n, per, blk, width,
           x_hbm, pos_hbm, wq_hbm, wk_hbm, wv_hbm, wo_hbm, gq_ref, gk_ref, freq_ref,
           xr_hbm, a_hbm,
           wq, wk, wv, wo, q_buf, k_buf, v_buf, x_buf, pos_buf, c_tab, s_tab, r_q, r_k,
           w_sem, own_sem, ld_sem, aloc_sem, x_send, x_recv, p_send, p_recv, a_send, a_recv):
    chips = n // 2
    ch = 2 * blk
    seq = n * blk
    heads = width // HEAD_DIM
    tiles = width // TN
    per_tile = TN // HEAD_DIM
    me = lax.axis_index('sp')
    my_chip = me // 2
    my_core = me % 2
    sib = 2 * my_chip + (1 - my_core)

    weights = [(wq_hbm, wq), (wk_hbm, wk), (wv_hbm, wv), (wo_hbm, wo)]

    def weight_copy(i):
        return pltpu.make_async_copy(weights[i][0], weights[i][1], w_sem.at[i])

    barrier = pltpu.get_barrier_semaphore()
    for d in range(1, n):
        pl.semaphore_signal(barrier, inc=1, device_id={'sp': lax.rem(me + d, n)},
                            device_id_type=pl.DeviceIdType.MESH)
    own_pos = pltpu.make_async_copy(pos_hbm.at[me], pos_buf.at[me], own_sem)
    own_pos.start()
    for i in range(4):
        weight_copy(i).start()
    pl.semaphore_wait(barrier, n - 1)

    partners = [(0, 1)] + [(dc, fl) for dc in ([1, chips - 1] + list(range(2, chips - 1))) for fl in (0, 1)]

    def partner(dc, fl):
        core = my_core if fl == 0 else 1 - my_core
        return 2 * lax.rem(my_chip + dc, chips) + core

    def x_copy(pi, s):
        tgt = partner(*partners[pi])
        return pltpu.make_async_remote_copy(
            src_ref=x_hbm.at[tgt * per + s], dst_ref=xr_hbm.at[s, me],
            send_sem=x_send.at[s, pi], recv_sem=x_recv.at[s, me],
            device_id={'sp': tgt}, device_id_type=pl.DeviceIdType.MESH)

    def pos_copy(pi):
        tgt = partner(*partners[pi])
        return pltpu.make_async_remote_copy(
            src_ref=pos_hbm.at[tgt], dst_ref=pos_buf.at[me],
            send_sem=p_send.at[pi], recv_sem=p_recv.at[me],
            device_id={'sp': tgt}, device_id_type=pl.DeviceIdType.MESH)

    for pi in range(n - 1):
        pos_copy(pi).start()
    for s in range(per):
        for pi in range(n - 1):
            x_copy(pi, s).start()
    own_pos.wait()

    def wait_x(s, src):
        pltpu.make_async_remote_copy(
            src_ref=x_hbm.at[0], dst_ref=xr_hbm.at[s, src], send_sem=x_send.at[s, 0],
            recv_sem=x_recv.at[s, src], device_id={'sp': sib},
            device_id_type=pl.DeviceIdType.MESH).wait_recv()

    def wait_pos(src):
        pltpu.make_async_remote_copy(
            src_ref=pos_hbm.at[0], dst_ref=pos_buf.at[src], send_sem=p_send.at[0],
            recv_sem=p_recv.at[src], device_id={'sp': sib},
            device_id_type=pl.DeviceIdType.MESH).wait_recv()

    def half_copy(src, slot, half):
        return pltpu.make_async_copy(
            src, x_buf.at[slot, pl.ds(pl.multiple_of(half * blk, blk), blk)], ld_sem.at[slot, half])

    def load_own(s, slot):
        half_copy(x_hbm.at[me * per + s], slot, my_core).start()
        wait_x(s, sib)
        half_copy(xr_hbm.at[s, sib], slot, 1 - my_core).start()

    def load_other(s, c, slot):
        for half in range(2):
            wait_x(s, 2 * c + half)
            half_copy(xr_hbm.at[s, 2 * c + half], slot, half).start()

    def wait_load(slot):
        for half in range(2):
            half_copy(xr_hbm.at[0, 0], slot, half).wait()

    n_own = per
    chip_offsets = [1, chips - 1] + list(range(2, chips - 1))

    def offset_of(i):
        out = jnp.int32(chip_offsets[0])
        for j in range(1, len(chip_offsets)):
            out = jnp.where(i == j, jnp.int32(chip_offsets[j]), out)
        return out

    lane = lax.broadcasted_iota(jnp.int32, (blk, HEAD_DIM), 1)
    row = lax.broadcasted_iota(jnp.int32, (blk, HEAD_DIM), 0)

    def tables(s, c):
        for half in range(2):
            p_row = pos_buf[2 * c + half, s, 0:1, :]
            sel = jnp.where(lane == row, jnp.broadcast_to(p_row, (blk, HEAD_DIM)), 0)
            p_col = jnp.sum(sel.astype(F32), axis=1, keepdims=True)
            ang = p_col * freq_ref[...]
            rows = pl.ds(half * blk, blk)
            c_tab[rows, :] = jnp.cos(ang)
            sn = jnp.sin(ang)
            s_tab[rows, :] = jnp.where(lane < HALF, -sn, sn)

    def rope_heads(buf, row0, r_ref, g_ref, j):
        for hh in range(per_tile):
            cols = pl.ds(pl.multiple_of(j * TN + hh * HEAD_DIM, HEAD_DIM), HEAD_DIM)
            u = buf[pl.ds(row0, ch), cols].astype(F32) * r_ref[...] * g_ref[0:1, cols].astype(F32)
            rot = pltpu.roll(u, HALF, 1)
            buf[pl.ds(row0, ch), cols] = (u * c_tab[...] + rot * s_tab[...]).astype(BF16)

    def proj_tile(x, w, dst, row0, j, acc):
        cols = pl.ds(pl.multiple_of(j * TN, TN), TN)
        p = jnp.dot(x[...], w[:, cols], preferred_element_type=F32).astype(BF16)
        dst[pl.ds(row0, ch), cols] = p
        if acc is None:
            return None
        pf = p.astype(F32)
        sq = pf * pf
        for t in range(per_tile):
            acc = acc + sq[:, t * HEAD_DIM:(t + 1) * HEAD_DIM]
        return acc

    def inv_rms(acc):
        ss = jnp.sum(acc, axis=1, keepdims=True)
        return jnp.broadcast_to(lax.rsqrt(ss * (1.0 / width) + NORM_EPS), (ch, HEAD_DIM))

    def qkv_chunk(s, c, slot, first, prefetch):
        row0 = pl.multiple_of(s * seq + c * ch, ch)
        x = x_buf.at[slot]
        wait_load(slot)
        tables(s, c)

        @pl.when(first)
        def _():
            weight_copy(0).wait()

        zero = jnp.zeros((ch, HEAD_DIM), F32)
        acc = lax.fori_loop(0, tiles, lambda j, acc: proj_tile(x, wq, q_buf, row0, j, acc), zero)
        r_q[...] = inv_rms(acc)

        @pl.when(first)
        def _():
            weight_copy(1).wait()

        def k_step(j, acc):
            acc = proj_tile(x, wk, k_buf, row0, j, acc)
            rope_heads(q_buf, row0, r_q, gq_ref, j)
            return acc
        acc = lax.fori_loop(0, tiles, k_step, zero)
        r_k[...] = inv_rms(acc)

        @pl.when(first)
        def _():
            weight_copy(2).wait()

        prefetch()

        def v_step(j, carry):
            proj_tile(x, wv, v_buf, row0, j, None)
            rope_heads(k_buf, row0, r_k, gk_ref, j)
            return carry
        lax.fori_loop(0, tiles, v_step, 0)

    dr = lax.broadcasted_iota(jnp.int32, (ch, ch), 0)
    dc_ = lax.broadcasted_iota(jnp.int32, (ch, ch), 1)
    diag_mask = dc_ <= dr
    nt = (((1,), (1,)), ((), ()))

    def attend(s):
        base = pl.multiple_of(s * seq, seq)

        def head(h, carry):
            cols = pl.ds(pl.multiple_of(h * HEAD_DIM, HEAD_DIM), HEAD_DIM)
            for i in range(chips):
                rows = pl.ds(base + i * ch, ch)
                q = q_buf[rows, cols]
                kd = k_buf[rows, cols]
                sd = lax.dot_general(q, kd, nt, preferred_element_type=F32)
                sd = jnp.where(diag_mask, sd, NEG)
                m = jnp.max(sd, axis=1, keepdims=True)
                if i:
                    past = pl.ds(base, i * ch)
                    sp_ = lax.dot_general(q, k_buf[past, cols], nt, preferred_element_type=F32)
                    m = jnp.maximum(m, jnp.max(sp_, axis=1, keepdims=True))
                ms = m * EXP2_SCALE
                ed = jnp.exp2(sd * EXP2_SCALE - ms)
                l = jnp.sum(ed, axis=1, keepdims=True)
                if i:
                    ep = jnp.exp2(sp_ * EXP2_SCALE - ms)
                    l = l + jnp.sum(ep, axis=1, keepdims=True)
                inv = 1.0 / l
                o = jnp.dot((ed * inv).astype(BF16), v_buf[rows, cols], preferred_element_type=F32)
                if i:
                    o = o + jnp.dot((ep * inv).astype(BF16), v_buf[past, cols], preferred_element_type=F32)
                q_buf[rows, cols] = o.astype(BF16)
            return carry
        lax.fori_loop(0, heads, head, 0)

    def a_rows(s, c, core):
        return k_buf.at[pl.ds(pl.multiple_of(s * seq + c * ch + core * blk, blk), blk)]

    def a_copy(s, c, core):
        tgt = 2 * c + core
        return pltpu.make_async_remote_copy(
            src_ref=a_rows(s, c, core), dst_ref=a_hbm.at[me * per + s],
            send_sem=a_send.at[s, tgt], recv_sem=a_recv.at[s, me],
            device_id={'sp': tgt}, device_id_type=pl.DeviceIdType.MESH)

    def a_local(s):
        return pltpu.make_async_copy(a_rows(s, my_chip, my_core), a_hbm.at[me * per + s], aloc_sem.at[s])

    def out_chunk(s, c):
        row0 = pl.multiple_of(s * seq + c * ch, ch)

        def step(j, carry):
            cols = pl.ds(pl.multiple_of(j * TN, TN), TN)
            k_buf[pl.ds(row0, ch), cols] = jnp.dot(
                q_buf[pl.ds(row0, ch), :], wo[:, cols], preferred_element_type=F32).astype(BF16)
            return carry
        lax.fori_loop(0, tiles, step, 0)

    def phase(s, carry):
        lo = jnp.where(s == 0, 0, n_own)
        start = jnp.where(s == 0, -n_own, 0)

        @pl.when(s == 0)
        def _():
            load_own(0, 0)

        @pl.when(s > 0)
        def _():
            load_other(s, lax.rem(my_chip + offset_of(0), chips), 0)

        def chunk(i, carry):
            own = i < 0
            sq = jnp.where(own, i + n_own, s)
            c = jnp.where(own, my_chip, lax.rem(my_chip + offset_of(i), chips))
            slot = lax.rem(i - start, 2)

            def prefetch():
                nxt = i + 1

                @pl.when(nxt < 0)
                def _():
                    load_own(nxt + n_own, 1 - slot)

                @pl.when(jnp.logical_and(nxt >= 0, nxt < chips - 1))
                def _():
                    load_other(s, lax.rem(my_chip + offset_of(nxt), chips), 1 - slot)

            @pl.when(jnp.logical_and(s == 0, i == -n_own))
            def _():
                for d in range(1, n):
                    wait_pos(lax.rem(me + d, n))
            qkv_chunk(sq, c, slot, jnp.logical_and(s == 0, i == -n_own), prefetch)
            return carry
        lax.fori_loop(start, chips - 1, chunk, 0)

        attend(s)

        @pl.when(s == 0)
        def _():
            weight_copy(3).wait()

        def out_step(i, carry):
            c = jnp.where(i == chips - 1, my_chip, lax.rem(my_chip + offset_of(i), chips))
            out_chunk(s, c)
            for core in range(2):
                mine = jnp.logical_and(c == my_chip, core == my_core)

                @pl.when(mine)
                def _():
                    a_local(s).start()

                @pl.when(jnp.logical_not(mine))
                def _():
                    a_copy(s, c, core).start()
            return carry
        lax.fori_loop(0, chips, out_step, 0)
        return carry

    lax.fori_loop(0, per, phase, 0)

    for s in range(per):
        a_local(s).wait()
        for pi in range(n - 1):
            x_copy(pi, s).wait_send()
            tgt = partner(*partners[pi])
            pltpu.make_async_remote_copy(
                src_ref=k_buf.at[pl.ds(0, blk)], dst_ref=a_hbm.at[tgt * per + s],
                send_sem=a_send.at[s, tgt], recv_sem=a_recv.at[s, tgt],
                device_id={'sp': tgt}, device_id_type=pl.DeviceIdType.MESH).wait()
    for pi in range(n - 1):
        pos_copy(pi).wait_send()


def exchange_attention(n, x_loc, pos_loc, w_query, w_key, w_value, w_out, gain_q, gain_k):
    batch, blk, width = x_loc.shape
    per = batch // n
    seq = n * blk
    freq = (1.0 / (np.float32(ROPE_THETA) ** (np.arange(0, HEAD_DIM, 2, dtype=np.float32) / np.float32(HEAD_DIM)))).astype(np.float32)
    freq = jnp.asarray(np.concatenate([freq, freq])[None, :])
    pos8 = jnp.broadcast_to(pos_loc.reshape(n, per, 1, blk), (n, per, 8, blk))
    hbm = pl.BlockSpec(memory_space=pl.ANY)
    vmem = pl.BlockSpec(memory_space=pltpu.VMEM)
    dma = pltpu.SemaphoreType.DMA
    wbuf = pltpu.VMEM((width, width), BF16)
    sbuf = pltpu.VMEM((per * seq, width), BF16)
    tab = pltpu.VMEM((2 * blk, HEAD_DIM), F32)
    _, a_all = pl.pallas_call(
        functools.partial(kernel, n, per, blk, width),
        out_shape=(jax.ShapeDtypeStruct((per, n, blk, width), BF16), jax.ShapeDtypeStruct((batch, blk, width), BF16)),
        in_specs=[hbm] * 6 + [vmem] * 3,
        out_specs=(hbm, hbm),
        scratch_shapes=[
            wbuf, wbuf, wbuf, wbuf, sbuf, sbuf, sbuf,
            pltpu.VMEM((2, 2 * blk, width), BF16),
            pltpu.VMEM((n, per, 8, blk), jnp.int32),
            tab, tab, tab, tab,
            dma((4,)), dma, dma((2, 2)), dma((per,)),
            dma((per, n)), dma((per, n)), dma((n,)), dma((n,)), dma((per, n)), dma((per, n)),
        ],
        compiler_params=pltpu.CompilerParams(
            collective_id=0, has_side_effects=True, vmem_limit_bytes=67043328),
        name='exchange_attention',
    )(x_loc, pos8, w_query, w_key, w_value, w_out, gain_q.reshape(1, width), gain_k.reshape(1, width), freq)
    return a_all


def solution(mesh):
    n = mesh.shape['sp']

    def local_block(x_loc, pos_loc, w_query, w_key, w_value, w_out, gain_q, gain_k, gain_out):
        a = exchange_attention(n, x_loc, pos_loc, w_query, w_key, w_value, w_out, gain_q, gain_k).astype(F32)
        mean_sq = jnp.mean(a * a, axis=-1, keepdims=True)
        return (x_loc.astype(F32) + a * lax.rsqrt(mean_sq + NORM_EPS) * gain_out.astype(F32)).astype(BF16)

    tok_spec = P('dp', 'sp', None)
    return jax.shard_map(local_block, mesh=mesh, in_specs=(tok_spec, P('dp', 'sp'), P(), P(), P(), P(), P(), P(), P()), out_specs=tok_spec, check_vma=False)
```

```python
import functools

import numpy as np
import jax
import jax.numpy as jnp
from jax import lax
from jax.experimental import pallas as pl
from jax.experimental.pallas import tpu as pltpu
from jax.sharding import PartitionSpec as P

HEAD_DIM = 128
HALF = HEAD_DIM // 2
ROPE_THETA = 500000.0
NORM_EPS = 1e-6
SCALE = HEAD_DIM ** -0.5
EXP2_SCALE = SCALE * 1.4426950408889634
NEG = -1e30
TN = 512
F32 = jnp.float32
BF16 = jnp.bfloat16


def kernel(n, per, blk, width,
           x_hbm, pos_hbm, wq_hbm, wk_hbm, wv_hbm, wo_hbm, gq_ref, gk_ref, ga_ref, freq_ref,
           xr_hbm, a_hbm, y_hbm,
           wq, wk, wv, wo, q_buf, k_buf, vt_buf, x_buf, pos_buf, c_tab, s_tab, r_q, r_k, sc_buf, g_tab,
           w_sem, own_sem, ld_sem, aloc_sem, out_sem, x_send, x_recv, p_send, p_recv, a_send, a_recv):
    chips = n // 2
    ch = 2 * blk
    seq = n * blk
    heads = width // HEAD_DIM
    tiles = width // TN
    per_tile = TN // HEAD_DIM
    me = lax.axis_index('sp')
    my_chip = me // 2
    my_core = me % 2
    sib = 2 * my_chip + (1 - my_core)

    weights = [(wq_hbm, wq), (wk_hbm, wk), (wv_hbm, wv), (wo_hbm, wo)]

    def weight_copy(i):
        return pltpu.make_async_copy(weights[i][0], weights[i][1], w_sem.at[i])

    barrier = pltpu.get_barrier_semaphore()
    for d in range(1, n):
        pl.semaphore_signal(barrier, inc=1, device_id={'sp': lax.rem(me + d, n)},
                            device_id_type=pl.DeviceIdType.MESH)
    own_pos = pltpu.make_async_copy(pos_hbm, pos_buf.at[me], own_sem)
    own_pos.start()
    for i in range(4):
        weight_copy(i).start()
    pl.semaphore_wait(barrier, n - 1)

    partners = [(0, 1)] + [(dc, fl) for dc in ([1, chips - 1] + list(range(2, chips - 1))) for fl in (0, 1)]

    def partner(dc, fl):
        core = my_core if fl == 0 else 1 - my_core
        return 2 * lax.rem(my_chip + dc, chips) + core

    def x_copy(pi, s):
        tgt = partner(*partners[pi])
        return pltpu.make_async_remote_copy(
            src_ref=x_hbm.at[tgt * per + s], dst_ref=xr_hbm.at[s, me],
            send_sem=x_send.at[s, pi], recv_sem=x_recv.at[s, me],
            device_id={'sp': tgt}, device_id_type=pl.DeviceIdType.MESH)

    def pos_copy(pi):
        tgt = partner(*partners[pi])
        return pltpu.make_async_remote_copy(
            src_ref=pos_hbm, dst_ref=pos_buf.at[me],
            send_sem=p_send.at[pi], recv_sem=p_recv.at[me],
            device_id={'sp': tgt}, device_id_type=pl.DeviceIdType.MESH)

    for pi in range(n - 1):
        pos_copy(pi).start()
    for s in range(per):
        for pi in range(n - 1):
            x_copy(pi, s).start()
    own_pos.wait()
    for gi, g in enumerate((gq_ref, gk_ref, ga_ref)):
        g_tab[gi:gi + 1, :] = g[...].astype(F32).reshape(1, width)

    def wait_x(s, src):
        pltpu.make_async_remote_copy(
            src_ref=x_hbm.at[0], dst_ref=xr_hbm.at[s, src], send_sem=x_send.at[s, 0],
            recv_sem=x_recv.at[s, src], device_id={'sp': sib},
            device_id_type=pl.DeviceIdType.MESH).wait_recv()

    def wait_pos(src):
        pltpu.make_async_remote_copy(
            src_ref=pos_hbm, dst_ref=pos_buf.at[src], send_sem=p_send.at[0],
            recv_sem=p_recv.at[src], device_id={'sp': sib},
            device_id_type=pl.DeviceIdType.MESH).wait_recv()

    def half_copy(src, slot, half):
        return pltpu.make_async_copy(
            src, x_buf.at[slot, pl.ds(pl.multiple_of(half * blk, blk), blk)], ld_sem.at[slot, half])

    def load_own(s, slot):
        half_copy(x_hbm.at[me * per + s], slot, my_core).start()
        wait_x(s, sib)
        half_copy(xr_hbm.at[s, sib], slot, 1 - my_core).start()

    def load_other(s, c, slot):
        for half in range(2):
            wait_x(s, 2 * c + half)
            half_copy(xr_hbm.at[s, 2 * c + half], slot, half).start()

    def wait_load(slot):
        for half in range(2):
            half_copy(xr_hbm.at[0, 0], slot, half).wait()

    n_own = per
    chip_offsets = [1, chips - 1] + list(range(2, chips - 1))

    def offset_of(i):
        out = jnp.int32(chip_offsets[0])
        for j in range(1, len(chip_offsets)):
            out = jnp.where(i == j, jnp.int32(chip_offsets[j]), out)
        return out

    lane = lax.broadcasted_iota(jnp.int32, (blk, HEAD_DIM), 1)
    row = lax.broadcasted_iota(jnp.int32, (blk, HEAD_DIM), 0)

    def tables(s, c):
        for half in range(2):
            p_row = pos_buf[2 * c + half, pl.ds(me * per + s, 1), :]
            sel = jnp.where(lane == row, jnp.broadcast_to(p_row, (blk, HEAD_DIM)), 0)
            p_col = jnp.sum(sel.astype(F32), axis=1, keepdims=True)
            ang = p_col * freq_ref[...]
            rows = pl.ds(half * blk, blk)
            c_tab[rows, :] = jnp.cos(ang)
            sn = jnp.sin(ang)
            s_tab[rows, :] = jnp.where(lane < HALF, -sn, sn)

    def rope_heads(buf, row0, r_ref, gi, j):
        for hh in range(per_tile):
            cols = pl.ds(j * TN + hh * HEAD_DIM, HEAD_DIM)
            u = buf[pl.ds(row0, ch), cols].astype(F32) * r_ref[...] * g_tab[gi:gi + 1, cols]
            rot = pltpu.roll(u, HALF, 1)
            buf[pl.ds(row0, ch), cols] = (u * c_tab[...] + rot * s_tab[...]).astype(BF16)

    def proj_tile(x, w, dst, row0, j, acc):
        cols = pl.ds(j * TN, TN)
        p = jnp.dot(x[...], w[:, cols], preferred_element_type=F32).astype(BF16)
        dst[pl.ds(row0, ch), cols] = p
        pf = p.astype(F32)
        sq = pf * pf
        for t in range(per_tile):
            acc = acc + sq[:, t * HEAD_DIM:(t + 1) * HEAD_DIM]
        return acc

    def inv_rms(acc):
        ss = jnp.sum(acc, axis=1, keepdims=True)
        return jnp.broadcast_to(lax.rsqrt(ss * (1.0 / width) + NORM_EPS), (ch, HEAD_DIM))

    def qkv_chunk(s, c, slot, first, prefetch):
        row0 = pl.multiple_of(s * seq + c * ch, ch)
        x = x_buf.at[slot]
        wait_load(slot)
        tables(s, c)

        @pl.when(first)
        def _():
            weight_copy(0).wait()

        zero = jnp.zeros((ch, HEAD_DIM), F32)
        acc = zero
        for j in range(tiles):
            acc = proj_tile(x, wq, q_buf, row0, j, acc)
        r_q[...] = inv_rms(acc)

        @pl.when(first)
        def _():
            weight_copy(1).wait()

        acc = zero
        for j in range(tiles):
            acc = proj_tile(x, wk, k_buf, row0, j, acc)
            rope_heads(q_buf, row0, r_q, 0, j)
        r_k[...] = inv_rms(acc)

        @pl.when(first)
        def _():
            weight_copy(2).wait()

        prefetch()

        for j in range(tiles):
            cols = pl.ds(j * TN, TN)
            v = jnp.dot(x[...], wv[:, cols], preferred_element_type=F32)
            vt_buf[s, cols, pl.ds(pl.multiple_of(c * ch, ch), ch)] = v.T.astype(BF16)
            rope_heads(k_buf, row0, r_k, 1, j)

    dr = lax.broadcasted_iota(jnp.int32, (ch, ch), 0)
    dc_ = lax.broadcasted_iota(jnp.int32, (ch, ch), 1)
    diag_mask = dr <= dc_
    nt = (((1,), (1,)), ((), ()))

    groups = [(g, chips - 1 - g) for g in range(chips // 2)]

    def scores(s, h, gi):
        base = pl.multiple_of(s * seq, seq)
        cols = pl.ds(pl.multiple_of(h * HEAD_DIM, HEAD_DIM), HEAD_DIM)
        off = 0
        for i in groups[gi]:
            rows = pl.ds(base + i * ch, ch)
            q = q_buf[rows, cols]
            if i:
                sc_buf[gi % 2, off:off + i * ch, :] = lax.dot_general(
                    k_buf[pl.ds(base, i * ch), cols], q, nt, preferred_element_type=F32)
            sd = lax.dot_general(k_buf[rows, cols], q, nt, preferred_element_type=F32)
            sc_buf[gi % 2, off + i * ch:off + (i + 1) * ch, :] = jnp.where(diag_mask, sd, NEG)
            off += (i + 1) * ch

    def weigh(s, h, gi):
        base = pl.multiple_of(s * seq, seq)
        cols = pl.ds(pl.multiple_of(h * HEAD_DIM, HEAD_DIM), HEAD_DIM)
        off = 0
        for i in groups[gi]:
            sc = sc_buf[gi % 2, off:off + (i + 1) * ch, :]
            m = jnp.max(sc, axis=0, keepdims=True) * EXP2_SCALE
            e = jnp.exp2(sc * EXP2_SCALE - m)
            inv = 1.0 / jnp.sum(e, axis=0, keepdims=True)
            o = jnp.dot(vt_buf[s, cols, 0:(i + 1) * ch], (e * inv).astype(BF16), preferred_element_type=F32)
            q_buf[pl.ds(base + i * ch, ch), cols] = o.T.astype(BF16)
            off += (i + 1) * ch

    def attend(s):
        scores(s, 0, 0)

        def head(h, carry):
            for gi in range(len(groups)):
                if gi + 1 < len(groups):
                    scores(s, h, gi + 1)
                else:
                    scores(s, lax.rem(h + 1, heads), 0)
                weigh(s, h, gi)
            return carry
        lax.fori_loop(0, heads, head, 0)

    def a_rows(s, c, core):
        return k_buf.at[pl.ds(pl.multiple_of(s * seq + c * ch + core * blk, blk), blk)]

    def a_copy(s, c, core):
        tgt = 2 * c + core
        return pltpu.make_async_remote_copy(
            src_ref=a_rows(s, c, core), dst_ref=a_hbm.at[me * per + s],
            send_sem=a_send.at[s, tgt], recv_sem=a_recv.at[s, me],
            device_id={'sp': tgt}, device_id_type=pl.DeviceIdType.MESH)

    def a_local(s):
        return pltpu.make_async_copy(a_rows(s, my_chip, my_core), a_hbm.at[me * per + s], aloc_sem.at[s])

    def out_chunk(s, c):
        row0 = pl.multiple_of(s * seq + c * ch, ch)

        for j in range(tiles):
            cols = pl.ds(j * TN, TN)
            k_buf[pl.ds(row0, ch), cols] = jnp.dot(
                q_buf[pl.ds(row0, ch), :], wo[:, cols], preferred_element_type=F32).astype(BF16)

    def phase(s, carry):
        lo = jnp.where(s == 0, 0, n_own)
        start = jnp.where(s == 0, -n_own, 0)

        @pl.when(s == 0)
        def _():
            load_own(0, 0)

        @pl.when(s > 0)
        def _():
            load_other(s, lax.rem(my_chip + offset_of(0), chips), 0)

        def chunk(i, carry):
            own = i < 0
            sq = jnp.where(own, i + n_own, s)
            c = jnp.where(own, my_chip, lax.rem(my_chip + offset_of(i), chips))
            slot = lax.rem(i - start, 2)

            def prefetch():
                nxt = i + 1

                @pl.when(nxt < 0)
                def _():
                    load_own(nxt + n_own, 1 - slot)

                @pl.when(jnp.logical_and(nxt >= 0, nxt < chips - 1))
                def _():
                    load_other(s, lax.rem(my_chip + offset_of(nxt), chips), 1 - slot)

            @pl.when(jnp.logical_and(s == 0, i == -n_own))
            def _():
                for d in range(1, n):
                    wait_pos(lax.rem(me + d, n))
            qkv_chunk(sq, c, slot, jnp.logical_and(s == 0, i == -n_own), prefetch)
            return carry
        lax.fori_loop(start, chips - 1, chunk, 0)

        attend(s)

        @pl.when(s == 0)
        def _():
            weight_copy(3).wait()

        def out_step(i, carry):
            c = jnp.where(i == chips - 1, my_chip, lax.rem(my_chip + offset_of(i), chips))
            out_chunk(s, c)
            for core in range(2):
                mine = jnp.logical_and(c == my_chip, core == my_core)

                @pl.when(mine)
                def _():
                    a_local(s).start()

                @pl.when(jnp.logical_not(mine))
                def _():
                    a_copy(s, c, core).start()
            return carry
        lax.fori_loop(0, chips, out_step, 0)
        return carry

    lax.fori_loop(0, per, phase, 0)

    def a_arrival(s, src):
        return pltpu.make_async_remote_copy(
            src_ref=k_buf.at[pl.ds(0, blk)], dst_ref=a_hbm.at[src * per + s],
            send_sem=a_send.at[s, src], recv_sem=a_recv.at[s, src],
            device_id={'sp': sib}, device_id_type=pl.DeviceIdType.MESH)

    def source(t):
        s = t // n
        r = lax.rem(t, n)
        return s, lax.rem(me + r, n)

    def fin_loads(t, slot):
        s, src = source(t)
        return (pltpu.make_async_copy(a_hbm.at[src * per + s], x_buf.at[slot, pl.ds(0, blk)], ld_sem.at[slot, 0]),
                pltpu.make_async_copy(x_hbm.at[src * per + s], x_buf.at[slot, pl.ds(blk, blk)], ld_sem.at[slot, 1]))

    def fin_store(t, slot):
        s, src = source(t)
        return pltpu.make_async_copy(x_buf.at[slot, pl.ds(0, blk)], y_hbm.at[src * per + s], out_sem.at[slot])

    def fin_fetch(t, slot):
        s, src = source(t)

        @pl.when(src == me)
        def _():
            a_local(s).wait()

        @pl.when(src != me)
        def _():
            a_arrival(s, src).wait_recv()
        for cp in fin_loads(t, slot):
            cp.start()

    steps = per * n
    fin_fetch(0, 0)

    def fin_step(t, carry):
        slot = lax.rem(t, 2)

        @pl.when(t >= 1)
        def _():
            fin_store(t - 1, 1 - slot).wait()

        @pl.when(t + 1 < steps)
        def _():
            fin_fetch(t + 1, 1 - slot)
        for cp in fin_loads(t, slot):
            cp.wait()
        acc = jnp.zeros((blk, HEAD_DIM), F32)
        for h in range(heads):
            v = x_buf[slot, 0:blk, h * HEAD_DIM:(h + 1) * HEAD_DIM].astype(F32)
            acc = acc + v * v
        r = lax.rsqrt(jnp.sum(acc, axis=1, keepdims=True) * (1.0 / width) + NORM_EPS)
        for h in range(heads):
            cols = slice(h * HEAD_DIM, (h + 1) * HEAD_DIM)
            v = x_buf[slot, 0:blk, cols].astype(F32) * r * g_tab[2:3, cols]
            x_buf[slot, 0:blk, cols] = (x_buf[slot, blk:2 * blk, cols].astype(F32) + v).astype(BF16)
        fin_store(t, slot).start()
        return carry
    lax.fori_loop(0, steps, fin_step, 0)
    fin_store(steps - 1, (steps - 1) % 2).wait()

    for s in range(per):
        for pi in range(n - 1):
            x_copy(pi, s).wait_send()
            a_arrival(s, partner(*partners[pi])).wait_send()
    for pi in range(n - 1):
        pos_copy(pi).wait_send()


def exchange_attention(n, x_loc, pos_loc, w_query, w_key, w_value, w_out, gain_q, gain_k, gain_out):
    batch, blk, width = x_loc.shape
    per = batch // n
    seq = n * blk
    freq = (1.0 / (np.float32(ROPE_THETA) ** (np.arange(0, HEAD_DIM, 2, dtype=np.float32) / np.float32(HEAD_DIM)))).astype(np.float32)
    freq = jnp.asarray(np.concatenate([freq, freq])[None, :])
    hbm = pl.BlockSpec(memory_space=pl.ANY)
    vmem = pl.BlockSpec(memory_space=pltpu.VMEM)
    dma = pltpu.SemaphoreType.DMA
    wbuf = pltpu.VMEM((width, width), BF16)
    sbuf = pltpu.VMEM((per * seq, width), BF16)
    tab = pltpu.VMEM((2 * blk, HEAD_DIM), F32)
    return pl.pallas_call(
        functools.partial(kernel, n, per, blk, width),
        out_shape=(jax.ShapeDtypeStruct((per, n, blk, width), BF16), jax.ShapeDtypeStruct((batch, blk, width), BF16),
                   jax.ShapeDtypeStruct((batch, blk, width), BF16)),
        in_specs=[hbm] * 6 + [vmem] * 4,
        out_specs=(hbm, hbm, hbm),
        scratch_shapes=[
            wbuf, wbuf, wbuf, wbuf, sbuf, sbuf, pltpu.VMEM((per, width, seq), BF16),
            pltpu.VMEM((2, 2 * blk, width), BF16),
            pltpu.VMEM((n, batch, blk), jnp.int32),
            tab, tab, tab, tab,
            pltpu.VMEM((2, seq + 2 * blk, 2 * blk), F32), pltpu.VMEM((3, width), F32),
            dma((4,)), dma, dma((2, 2)), dma((per,)), dma((2,)),
            dma((per, n)), dma((per, n)), dma((n,)), dma((n,)), dma((per, n)), dma((per, n)),
        ],
        compiler_params=pltpu.CompilerParams(
            collective_id=0, has_side_effects=True, vmem_limit_bytes=67043328),
        name='exchange_attention',
    )(x_loc, pos_loc, w_query, w_key, w_value, w_out, gain_q, gain_k, gain_out, freq)[2]


def solution(mesh):
    n = mesh.shape['sp']

    def local_block(x_loc, pos_loc, w_query, w_key, w_value, w_out, gain_q, gain_k, gain_out):
        return exchange_attention(n, x_loc, pos_loc, w_query, w_key, w_value, w_out, gain_q, gain_k, gain_out)

    tok_spec = P('dp', 'sp', None)
    return jax.shard_map(local_block, mesh=mesh, in_specs=(tok_spec, P('dp', 'sp'), P(), P(), P(), P(), P(), P(), P()), out_specs=tok_spec, check_vma=False)
```

```python
import functools

import numpy as np
import jax
import jax.numpy as jnp
from jax import lax
from jax.experimental import pallas as pl
from jax.experimental.pallas import tpu as pltpu
from jax.sharding import PartitionSpec as P

HEAD_DIM = 128
HALF = HEAD_DIM // 2
ROPE_THETA = 500000.0
NORM_EPS = 1e-6
SCALE = HEAD_DIM ** -0.5
EXP2_SCALE = SCALE * 1.4426950408889634
NEG = -1e30
TN = 512
UNROLL = 4
F32 = jnp.float32
BF16 = jnp.bfloat16


def kernel(n, per, blk, width,
           x_hbm, pos_hbm, wq_hbm, wk_hbm, wv_hbm, wo_hbm, gq_ref, gk_ref, ga_ref, freq_ref,
           xr_hbm, a_hbm, y_hbm,
           wq, wk, wv, wo, q_buf, k_buf, vt_buf, x_buf, pos_buf, c_tab, s_tab, r_q, r_k, sc_buf, o_buf, g_tab,
           w_sem, own_sem, ld_sem, aloc_sem, out_sem, x_send, x_recv, p_send, p_recv, a_send, a_recv):
    chips = n // 2
    ch = 2 * blk
    seq = n * blk
    heads = width // HEAD_DIM
    tiles = width // TN
    per_tile = TN // HEAD_DIM
    me = lax.axis_index('sp')
    my_chip = me // 2
    my_core = me % 2
    sib = 2 * my_chip + (1 - my_core)

    weights = [(wq_hbm, wq), (wk_hbm, wk), (wv_hbm, wv), (wo_hbm, wo)]

    def weight_copy(i):
        return pltpu.make_async_copy(weights[i][0], weights[i][1], w_sem.at[i])

    barrier = pltpu.get_barrier_semaphore()
    for d in range(1, n):
        pl.semaphore_signal(barrier, inc=1, device_id={'sp': lax.rem(me + d, n)},
                            device_id_type=pl.DeviceIdType.MESH)
    own_pos = pltpu.make_async_copy(pos_hbm, pos_buf.at[me], own_sem)
    own_pos.start()
    for i in range(4):
        weight_copy(i).start()
    pl.semaphore_wait(barrier, n - 1)

    partners = [(0, 1)] + [(dc, fl) for dc in ([1, chips - 1] + list(range(2, chips - 1))) for fl in (0, 1)]

    def partner(dc, fl):
        core = my_core if fl == 0 else 1 - my_core
        return 2 * lax.rem(my_chip + dc, chips) + core

    def x_copy(pi, s):
        tgt = partner(*partners[pi])
        return pltpu.make_async_remote_copy(
            src_ref=x_hbm.at[tgt * per + s], dst_ref=xr_hbm.at[s, me],
            send_sem=x_send.at[s, pi], recv_sem=x_recv.at[s, me],
            device_id={'sp': tgt}, device_id_type=pl.DeviceIdType.MESH)

    def pos_copy(pi):
        tgt = partner(*partners[pi])
        return pltpu.make_async_remote_copy(
            src_ref=pos_hbm, dst_ref=pos_buf.at[me],
            send_sem=p_send.at[pi], recv_sem=p_recv.at[me],
            device_id={'sp': tgt}, device_id_type=pl.DeviceIdType.MESH)

    for pi in range(n - 1):
        pos_copy(pi).start()
    for s in range(per):
        for pi in range(n - 1):
            x_copy(pi, s).start()
    own_pos.wait()
    for gi, g in enumerate((gq_ref, gk_ref, ga_ref)):
        g_tab[gi:gi + 1, :] = g[...].astype(F32).reshape(1, width)

    def wait_x(s, src):
        pltpu.make_async_remote_copy(
            src_ref=x_hbm.at[0], dst_ref=xr_hbm.at[s, src], send_sem=x_send.at[s, 0],
            recv_sem=x_recv.at[s, src], device_id={'sp': sib},
            device_id_type=pl.DeviceIdType.MESH).wait_recv()

    def wait_pos(src):
        pltpu.make_async_remote_copy(
            src_ref=pos_hbm, dst_ref=pos_buf.at[src], send_sem=p_send.at[0],
            recv_sem=p_recv.at[src], device_id={'sp': sib},
            device_id_type=pl.DeviceIdType.MESH).wait_recv()

    def half_copy(src, slot, half):
        return pltpu.make_async_copy(
            src, x_buf.at[slot, pl.ds(pl.multiple_of(half * blk, blk), blk)], ld_sem.at[slot, half])

    def load_own(s, slot):
        half_copy(x_hbm.at[me * per + s], slot, my_core).start()
        wait_x(s, sib)
        half_copy(xr_hbm.at[s, sib], slot, 1 - my_core).start()

    def load_other(s, c, slot):
        for half in range(2):
            wait_x(s, 2 * c + half)
            half_copy(xr_hbm.at[s, 2 * c + half], slot, half).start()

    def wait_load(slot):
        for half in range(2):
            half_copy(xr_hbm.at[0, 0], slot, half).wait()

    n_own = per
    chip_offsets = [1, chips - 1] + list(range(2, chips - 1))

    def offset_of(i):
        out = jnp.int32(chip_offsets[0])
        for j in range(1, len(chip_offsets)):
            out = jnp.where(i == j, jnp.int32(chip_offsets[j]), out)
        return out

    lane = lax.broadcasted_iota(jnp.int32, (blk, HEAD_DIM), 1)
    row = lax.broadcasted_iota(jnp.int32, (blk, HEAD_DIM), 0)

    def tables(s, c):
        for half in range(2):
            p_row = pos_buf[2 * c + half, pl.ds(me * per + s, 1), :]
            sel = jnp.where(lane == row, jnp.broadcast_to(p_row, (blk, HEAD_DIM)), 0)
            p_col = jnp.sum(sel.astype(F32), axis=1, keepdims=True)
            ang = p_col * freq_ref[...]
            rows = pl.ds(half * blk, blk)
            c_tab[rows, :] = jnp.cos(ang)
            sn = jnp.sin(ang)
            s_tab[rows, :] = jnp.where(lane < HALF, -sn, sn)

    def rope_heads(buf, row0, r_ref, gi, j):
        for hh in range(per_tile):
            cols = pl.ds(j * TN + hh * HEAD_DIM, HEAD_DIM)
            u = buf[pl.ds(row0, ch), cols].astype(F32) * r_ref[...] * g_tab[gi:gi + 1, cols]
            rot = pltpu.roll(u, HALF, 1)
            buf[pl.ds(row0, ch), cols] = (u * c_tab[...] + rot * s_tab[...]).astype(BF16)

    def proj_tile(x, w, dst, row0, j, acc):
        cols = pl.ds(j * TN, TN)
        p = jnp.dot(x[...], w[:, cols], preferred_element_type=F32).astype(BF16)
        dst[pl.ds(row0, ch), cols] = p
        pf = p.astype(F32)
        sq = pf * pf
        for t in range(per_tile):
            acc = acc + sq[:, t * HEAD_DIM:(t + 1) * HEAD_DIM]
        return acc

    def inv_rms(acc):
        ss = jnp.sum(acc, axis=1, keepdims=True)
        return jnp.broadcast_to(lax.rsqrt(ss * (1.0 / width) + NORM_EPS), (ch, HEAD_DIM))

    def qkv_chunk(s, c, slot, first, prefetch):
        row0 = pl.multiple_of(s * seq + c * ch, ch)
        x = x_buf.at[slot]
        wait_load(slot)
        tables(s, c)

        @pl.when(first)
        def _():
            weight_copy(0).wait()

        zero = jnp.zeros((ch, HEAD_DIM), F32)
        acc = zero
        for j in range(tiles):
            acc = proj_tile(x, wq, q_buf, row0, j, acc)
        r_q[...] = inv_rms(acc)

        @pl.when(first)
        def _():
            weight_copy(1).wait()

        acc = zero
        for j in range(tiles):
            acc = proj_tile(x, wk, k_buf, row0, j, acc)
            rope_heads(q_buf, row0, r_q, 0, j)
        r_k[...] = inv_rms(acc)

        @pl.when(first)
        def _():
            weight_copy(2).wait()

        prefetch()

        for j in range(tiles):
            cols = pl.ds(j * TN, TN)
            v = jnp.dot(x[...], wv[:, cols], preferred_element_type=F32)
            vt_buf[s, cols, pl.ds(pl.multiple_of(c * ch, ch), ch)] = v.T.astype(BF16)
            rope_heads(k_buf, row0, r_k, 1, j)

    dr = lax.broadcasted_iota(jnp.int32, (ch, ch), 0)
    dc_ = lax.broadcasted_iota(jnp.int32, (ch, ch), 1)
    diag_mask = dr <= dc_
    nt = (((1,), (1,)), ((), ()))

    def scores(s, i, h, slot):
        base = pl.multiple_of(s * seq, seq)
        cols = pl.ds(pl.multiple_of(h * HEAD_DIM, HEAD_DIM), HEAD_DIM)
        rows = pl.ds(base + i * ch, ch)
        q = q_buf[rows, cols]
        if i:
            sc_buf[slot, 0:i * ch, :] = lax.dot_general(
                k_buf[pl.ds(base, i * ch), cols], q, nt, preferred_element_type=F32)
        sd = lax.dot_general(k_buf[rows, cols], q, nt, preferred_element_type=F32)
        sc_buf[slot, i * ch:(i + 1) * ch, :] = jnp.where(diag_mask, sd, NEG)

    def weigh(s, i, h, slot):
        base = pl.multiple_of(s * seq, seq)
        cols = pl.ds(pl.multiple_of(h * HEAD_DIM, HEAD_DIM), HEAD_DIM)
        sc = sc_buf[slot, 0:(i + 1) * ch, :]
        m = jnp.max(sc, axis=0, keepdims=True) * EXP2_SCALE
        e = jnp.exp2(sc * EXP2_SCALE - m)
        inv = 1.0 / jnp.sum(e, axis=0, keepdims=True)
        o = jnp.dot(vt_buf[s, cols, 0:(i + 1) * ch], (e * inv).astype(BF16), preferred_element_type=F32)
        o_buf[:, cols] = o.T.astype(BF16)

    def attend(s, i):
        scores(s, i, 0, 0)

        def some(g, carry):
            for u in range(UNROLL):
                scores(s, i, lax.rem(UNROLL * g + u + 1, heads), (u + 1) % 2)
                weigh(s, i, UNROLL * g + u, u % 2)
            return carry
        lax.fori_loop(0, heads // UNROLL, some, 0)

    def a_rows(s, c, core):
        return q_buf.at[pl.ds(pl.multiple_of(s * seq + c * ch + core * blk, blk), blk)]

    def a_copy(s, c, core):
        tgt = 2 * c + core
        return pltpu.make_async_remote_copy(
            src_ref=a_rows(s, c, core), dst_ref=a_hbm.at[me * per + s],
            send_sem=a_send.at[s, tgt], recv_sem=a_recv.at[s, me],
            device_id={'sp': tgt}, device_id_type=pl.DeviceIdType.MESH)

    def a_local(s):
        return pltpu.make_async_copy(a_rows(s, my_chip, my_core), a_hbm.at[me * per + s], aloc_sem.at[s])

    def out_chunk(s, c):
        row0 = pl.multiple_of(s * seq + c * ch, ch)

        for j in range(tiles):
            cols = pl.ds(j * TN, TN)
            q_buf[pl.ds(row0, ch), cols] = jnp.dot(
                o_buf[...], wo[:, cols], preferred_element_type=F32).astype(BF16)

    def phase(s, carry):
        lo = jnp.where(s == 0, 0, n_own)
        start = jnp.where(s == 0, -n_own, 0)

        @pl.when(s == 0)
        def _():
            load_own(0, 0)

        @pl.when(s > 0)
        def _():
            load_other(s, lax.rem(my_chip + offset_of(0), chips), 0)

        def chunk(i, carry):
            own = i < 0
            sq = jnp.where(own, i + n_own, s)
            c = jnp.where(own, my_chip, lax.rem(my_chip + offset_of(i), chips))
            slot = lax.rem(i - start, 2)

            def prefetch():
                nxt = i + 1

                @pl.when(nxt < 0)
                def _():
                    load_own(nxt + n_own, 1 - slot)

                @pl.when(jnp.logical_and(nxt >= 0, nxt < chips - 1))
                def _():
                    load_other(s, lax.rem(my_chip + offset_of(nxt), chips), 1 - slot)

            @pl.when(jnp.logical_and(s == 0, i == -n_own))
            def _():
                for d in range(1, n):
                    wait_pos(lax.rem(me + d, n))
            qkv_chunk(sq, c, slot, jnp.logical_and(s == 0, i == -n_own), prefetch)
            return carry
        lax.fori_loop(start, chips - 1, chunk, 0)

        @pl.when(s == 0)
        def _():
            weight_copy(3).wait()

        def out_step(i, carry):
            c = jnp.where(i == chips - 1, my_chip, lax.rem(my_chip + offset_of(i), chips))
            for blk_i in range(chips):
                @pl.when(c == blk_i)
                def _():
                    attend(s, blk_i)
            out_chunk(s, c)
            for core in range(2):
                mine = jnp.logical_and(c == my_chip, core == my_core)

                @pl.when(mine)
                def _():
                    a_local(s).start()

                @pl.when(jnp.logical_not(mine))
                def _():
                    a_copy(s, c, core).start()
            return carry
        lax.fori_loop(0, chips, out_step, 0)
        return carry

    lax.fori_loop(0, per, phase, 0)

    home = [(0, 1)] + [(dc, fl) for fl in (0, 1) for dc in (chips - 1, 1)] + partners[5:]

    def a_arrival(s, src):
        return pltpu.make_async_remote_copy(
            src_ref=q_buf.at[pl.ds(0, blk)], dst_ref=a_hbm.at[src * per + s],
            send_sem=a_send.at[s, src], recv_sem=a_recv.at[s, src],
            device_id={'sp': sib}, device_id_type=pl.DeviceIdType.MESH)

    def source(t):
        s = t // n
        r = lax.rem(t, n)
        src = me
        for k, (dc, fl) in enumerate(home):
            src = jnp.where(r == k + 1, partner(dc, fl), src)
        return s, src

    def fin_loads(t, slot):
        s, src = source(t)
        return (pltpu.make_async_copy(a_hbm.at[src * per + s], x_buf.at[slot, pl.ds(0, blk)], ld_sem.at[slot, 0]),
                pltpu.make_async_copy(x_hbm.at[src * per + s], x_buf.at[slot, pl.ds(blk, blk)], ld_sem.at[slot, 1]))

    def fin_store(t, slot):
        s, src = source(t)
        return pltpu.make_async_copy(x_buf.at[slot, pl.ds(0, blk)], y_hbm.at[src * per + s], out_sem.at[slot])

    def fin_fetch(t, slot):
        s, src = source(t)

        @pl.when(src == me)
        def _():
            a_local(s).wait()

        @pl.when(src != me)
        def _():
            a_arrival(s, src).wait_recv()
        for cp in fin_loads(t, slot):
            cp.start()

    steps = per * n
    fin_fetch(0, 0)

    def fin_step(t, carry):
        slot = lax.rem(t, 2)

        @pl.when(t >= 1)
        def _():
            fin_store(t - 1, 1 - slot).wait()

        @pl.when(t + 1 < steps)
        def _():
            fin_fetch(t + 1, 1 - slot)
        for cp in fin_loads(t, slot):
            cp.wait()
        acc = jnp.zeros((blk, HEAD_DIM), F32)
        for h in range(heads):
            v = x_buf[slot, 0:blk, h * HEAD_DIM:(h + 1) * HEAD_DIM].astype(F32)
            acc = acc + v * v
        r = lax.rsqrt(jnp.sum(acc, axis=1, keepdims=True) * (1.0 / width) + NORM_EPS)
        for h in range(heads):
            cols = slice(h * HEAD_DIM, (h + 1) * HEAD_DIM)
            v = x_buf[slot, 0:blk, cols].astype(F32) * r * g_tab[2:3, cols]
            x_buf[slot, 0:blk, cols] = (x_buf[slot, blk:2 * blk, cols].astype(F32) + v).astype(BF16)
        fin_store(t, slot).start()
        return carry
    lax.fori_loop(0, steps, fin_step, 0)
    fin_store(steps - 1, (steps - 1) % 2).wait()

    for s in range(per):
        for pi in range(n - 1):
            x_copy(pi, s).wait_send()
            a_arrival(s, partner(*partners[pi])).wait_send()
    for pi in range(n - 1):
        pos_copy(pi).wait_send()


def exchange_attention(n, x_loc, pos_loc, w_query, w_key, w_value, w_out, gain_q, gain_k, gain_out):
    batch, blk, width = x_loc.shape
    per = batch // n
    seq = n * blk
    freq = (1.0 / (np.float32(ROPE_THETA) ** (np.arange(0, HEAD_DIM, 2, dtype=np.float32) / np.float32(HEAD_DIM)))).astype(np.float32)
    freq = jnp.asarray(np.concatenate([freq, freq])[None, :])
    hbm = pl.BlockSpec(memory_space=pl.ANY)
    vmem = pl.BlockSpec(memory_space=pltpu.VMEM)
    dma = pltpu.SemaphoreType.DMA
    wbuf = pltpu.VMEM((width, width), BF16)
    sbuf = pltpu.VMEM((per * seq, width), BF16)
    tab = pltpu.VMEM((2 * blk, HEAD_DIM), F32)
    return pl.pallas_call(
        functools.partial(kernel, n, per, blk, width),
        out_shape=(jax.ShapeDtypeStruct((per, n, blk, width), BF16), jax.ShapeDtypeStruct((batch, blk, width), BF16),
                   jax.ShapeDtypeStruct((batch, blk, width), BF16)),
        in_specs=[hbm] * 6 + [vmem] * 4,
        out_specs=(hbm, hbm, hbm),
        scratch_shapes=[
            wbuf, wbuf, wbuf, wbuf, sbuf, sbuf, pltpu.VMEM((per, width, seq), BF16),
            pltpu.VMEM((2, 2 * blk, width), BF16),
            pltpu.VMEM((n, batch, blk), jnp.int32),
            tab, tab, tab, tab,
            pltpu.VMEM((2, seq, 2 * blk), F32), pltpu.VMEM((2 * blk, width), BF16), pltpu.VMEM((3, width), F32),
            dma((4,)), dma, dma((2, 2)), dma((per,)), dma((2,)),
            dma((per, n)), dma((per, n)), dma((n,)), dma((n,)), dma((per, n)), dma((per, n)),
        ],
        compiler_params=pltpu.CompilerParams(
            collective_id=0, has_side_effects=True, vmem_limit_bytes=67043328),
        name='exchange_attention',
    )(x_loc, pos_loc, w_query, w_key, w_value, w_out, gain_q, gain_k, gain_out, freq)[2]


def solution(mesh):
    n = mesh.shape['sp']

    def local_block(x_loc, pos_loc, w_query, w_key, w_value, w_out, gain_q, gain_k, gain_out):
        return exchange_attention(n, x_loc, pos_loc, w_query, w_key, w_value, w_out, gain_q, gain_k, gain_out)

    tok_spec = P('dp', 'sp', None)
    return jax.shard_map(local_block, mesh=mesh, in_specs=(tok_spec, P('dp', 'sp'), P(), P(), P(), P(), P(), P(), P()), out_specs=tok_spec, check_vma=False)
```

```python
import functools

import numpy as np
import jax
import jax.numpy as jnp
from jax import lax
from jax.experimental import pallas as pl
from jax.experimental.pallas import tpu as pltpu
from jax.sharding import PartitionSpec as P

HEAD_DIM = 128
HALF = HEAD_DIM // 2
ROPE_THETA = 500000.0
NORM_EPS = 1e-6
SCALE = HEAD_DIM ** -0.5
EXP2_SCALE = SCALE * 1.4426950408889634
NEG = -1e30
TN = 512
UNROLL = 4
F32 = jnp.float32
BF16 = jnp.bfloat16


def kernel(n, per, blk, width,
           x_hbm, pos_hbm, wq_hbm, wk_hbm, wv_hbm, wo_hbm, gq_ref, gk_ref, ga_ref, freq_ref,
           xr_hbm, a_hbm, y_hbm,
           wq, wk, wv, wo, q_buf, k_buf, vt_buf, x_buf, pos_buf, c_tab, s_tab, r_q, r_k, sc_buf, o_buf, g_tab,
           w_sem, own_sem, ld_sem, aloc_sem, out_sem, x_send, x_recv, p_send, p_recv, a_send, a_recv):
    chips = n // 2
    ch = 2 * blk
    seq = n * blk
    heads = width // HEAD_DIM
    tiles = width // TN
    per_tile = TN // HEAD_DIM
    me = lax.axis_index('sp')
    my_chip = me // 2
    my_core = me % 2
    sib = 2 * my_chip + (1 - my_core)

    weights = [(wq_hbm, wq), (wk_hbm, wk), (wv_hbm, wv), (wo_hbm, wo)]

    def weight_copy(i):
        return pltpu.make_async_copy(weights[i][0], weights[i][1], w_sem.at[i])

    barrier = pltpu.get_barrier_semaphore()
    for d in range(1, n):
        pl.semaphore_signal(barrier, inc=1, device_id={'sp': lax.rem(me + d, n)},
                            device_id_type=pl.DeviceIdType.MESH)
    own_pos = pltpu.make_async_copy(pos_hbm, pos_buf.at[me], own_sem)
    own_pos.start()
    first_own = pltpu.make_async_copy(
        x_hbm.at[me * per], x_buf.at[0, pl.ds(pl.multiple_of(my_core * blk, blk), blk)], ld_sem.at[0, my_core])
    first_own.start()
    weight_copy(0).start()
    pl.semaphore_wait(barrier, n - 1)

    partners = [(0, 1)] + [(dc, fl) for dc in ([1, chips - 1] + list(range(2, chips - 1))) for fl in (0, 1)]

    def partner(dc, fl):
        core = my_core if fl == 0 else 1 - my_core
        return 2 * lax.rem(my_chip + dc, chips) + core

    def x_copy(pi, s):
        tgt = partner(*partners[pi])
        return pltpu.make_async_remote_copy(
            src_ref=x_hbm.at[tgt * per + s], dst_ref=xr_hbm.at[s, me],
            send_sem=x_send.at[s, pi], recv_sem=x_recv.at[s, me],
            device_id={'sp': tgt}, device_id_type=pl.DeviceIdType.MESH)

    def pos_copy(pi):
        tgt = partner(*partners[pi])
        return pltpu.make_async_remote_copy(
            src_ref=pos_hbm, dst_ref=pos_buf.at[me],
            send_sem=p_send.at[pi], recv_sem=p_recv.at[me],
            device_id={'sp': tgt}, device_id_type=pl.DeviceIdType.MESH)

    for pi in range(n - 1):
        pos_copy(pi).start()
    for s in range(per):
        for pi in range(n - 1):
            x_copy(pi, s).start()
    weight_copy(1).start()
    weight_copy(2).start()
    own_pos.wait()
    for gi, g in enumerate((gq_ref, gk_ref, ga_ref)):
        g_tab[gi:gi + 1, :] = g[...].astype(F32).reshape(1, width)

    def wait_x(s, src):
        pltpu.make_async_remote_copy(
            src_ref=x_hbm.at[0], dst_ref=xr_hbm.at[s, src], send_sem=x_send.at[s, 0],
            recv_sem=x_recv.at[s, src], device_id={'sp': sib},
            device_id_type=pl.DeviceIdType.MESH).wait_recv()

    def wait_pos(src):
        pltpu.make_async_remote_copy(
            src_ref=pos_hbm, dst_ref=pos_buf.at[src], send_sem=p_send.at[0],
            recv_sem=p_recv.at[src], device_id={'sp': sib},
            device_id_type=pl.DeviceIdType.MESH).wait_recv()

    def half_copy(src, slot, half):
        return pltpu.make_async_copy(
            src, x_buf.at[slot, pl.ds(pl.multiple_of(half * blk, blk), blk)], ld_sem.at[slot, half])

    def load_own(s, slot):
        half_copy(x_hbm.at[me * per + s], slot, my_core).start()
        wait_x(s, sib)
        half_copy(xr_hbm.at[s, sib], slot, 1 - my_core).start()

    def load_other(s, c, slot):
        for half in range(2):
            wait_x(s, 2 * c + half)
            half_copy(xr_hbm.at[s, 2 * c + half], slot, half).start()

    def wait_load(slot):
        for half in range(2):
            half_copy(xr_hbm.at[0, 0], slot, half).wait()

    n_own = per
    chip_offsets = [1, chips - 1] + list(range(2, chips - 1))

    def offset_of(i):
        out = jnp.int32(chip_offsets[0])
        for j in range(1, len(chip_offsets)):
            out = jnp.where(i == j, jnp.int32(chip_offsets[j]), out)
        return out

    lane = lax.broadcasted_iota(jnp.int32, (blk, HEAD_DIM), 1)
    row = lax.broadcasted_iota(jnp.int32, (blk, HEAD_DIM), 0)

    def tables(s, c):
        for half in range(2):
            p_row = pos_buf[2 * c + half, pl.ds(me * per + s, 1), :]
            sel = jnp.where(lane == row, jnp.broadcast_to(p_row, (blk, HEAD_DIM)), 0)
            p_col = jnp.sum(sel.astype(F32), axis=1, keepdims=True)
            ang = p_col * freq_ref[...]
            rows = pl.ds(half * blk, blk)
            c_tab[rows, :] = jnp.cos(ang)
            sn = jnp.sin(ang)
            s_tab[rows, :] = jnp.where(lane < HALF, -sn, sn)

    def rope_heads(buf, row0, r_ref, gi, j):
        for hh in range(per_tile):
            cols = pl.ds(j * TN + hh * HEAD_DIM, HEAD_DIM)
            u = buf[pl.ds(row0, ch), cols].astype(F32) * r_ref[...] * g_tab[gi:gi + 1, cols]
            rot = pltpu.roll(u, HALF, 1)
            buf[pl.ds(row0, ch), cols] = (u * c_tab[...] + rot * s_tab[...]).astype(BF16)

    def proj_tile(x, w, dst, row0, j, acc):
        cols = pl.ds(j * TN, TN)
        p = jnp.dot(x[...], w[:, cols], preferred_element_type=F32).astype(BF16)
        dst[pl.ds(row0, ch), cols] = p
        pf = p.astype(F32)
        sq = pf * pf
        for t in range(per_tile):
            acc = acc + sq[:, t * HEAD_DIM:(t + 1) * HEAD_DIM]
        return acc

    def inv_rms(acc):
        ss = jnp.sum(acc, axis=1, keepdims=True)
        return jnp.broadcast_to(lax.rsqrt(ss * (1.0 / width) + NORM_EPS), (ch, HEAD_DIM))

    def qkv_chunk(s, c, slot, first, prefetch):
        row0 = pl.multiple_of(s * seq + c * ch, ch)
        x = x_buf.at[slot]
        wait_load(slot)

        @pl.when(first)
        def _():
            weight_copy(0).wait()

        zero = jnp.zeros((ch, HEAD_DIM), F32)
        tables(s, c)
        acc = zero
        for j in range(tiles):
            acc = proj_tile(x, wq, q_buf, row0, j, acc)
        r_q[...] = inv_rms(acc)

        @pl.when(first)
        def _():
            weight_copy(1).wait()

        acc = zero
        for j in range(tiles):
            acc = proj_tile(x, wk, k_buf, row0, j, acc)
            rope_heads(q_buf, row0, r_q, 0, j)
        r_k[...] = inv_rms(acc)

        @pl.when(first)
        def _():
            weight_copy(2).wait()

        @pl.when(first)
        def _():
            weight_copy(3).start()

        prefetch()

        for j in range(tiles):
            cols = pl.ds(j * TN, TN)
            v = jnp.dot(x[...], wv[:, cols], preferred_element_type=F32)
            vt_buf[s, cols, pl.ds(pl.multiple_of(c * ch, ch), ch)] = v.T.astype(BF16)
            rope_heads(k_buf, row0, r_k, 1, j)

    dr = lax.broadcasted_iota(jnp.int32, (ch, ch), 0)
    dc_ = lax.broadcasted_iota(jnp.int32, (ch, ch), 1)
    diag_mask = dr <= dc_
    nt = (((1,), (1,)), ((), ()))

    def scores(s, i, h, slot):
        base = pl.multiple_of(s * seq, seq)
        cols = pl.ds(pl.multiple_of(h * HEAD_DIM, HEAD_DIM), HEAD_DIM)
        rows = pl.ds(base + i * ch, ch)
        q = q_buf[rows, cols]
        if i:
            sc_buf[slot, 0:i * ch, :] = lax.dot_general(
                k_buf[pl.ds(base, i * ch), cols], q, nt, preferred_element_type=F32)
        sd = lax.dot_general(k_buf[rows, cols], q, nt, preferred_element_type=F32)
        sc_buf[slot, i * ch:(i + 1) * ch, :] = jnp.where(diag_mask, sd, NEG)

    def weigh(s, i, h, slot):
        base = pl.multiple_of(s * seq, seq)
        cols = pl.ds(pl.multiple_of(h * HEAD_DIM, HEAD_DIM), HEAD_DIM)
        sc = sc_buf[slot, 0:(i + 1) * ch, :]
        m = jnp.max(sc, axis=0, keepdims=True) * EXP2_SCALE
        e = jnp.exp2(sc * EXP2_SCALE - m)
        inv = 1.0 / jnp.sum(e, axis=0, keepdims=True)
        o = jnp.dot(vt_buf[s, cols, 0:(i + 1) * ch], (e * inv).astype(BF16), preferred_element_type=F32)
        o_buf[:, cols] = o.T.astype(BF16)

    def attend(s, i):
        scores(s, i, 0, 0)

        def some(g, carry):
            for u in range(UNROLL):
                scores(s, i, lax.rem(UNROLL * g + u + 1, heads), (u + 1) % 2)
                weigh(s, i, UNROLL * g + u, u % 2)
            return carry
        lax.fori_loop(0, heads // UNROLL, some, 0)

    def a_rows(s, c, core):
        return q_buf.at[pl.ds(pl.multiple_of(s * seq + c * ch + core * blk, blk), blk)]

    def a_copy(s, c, core):
        tgt = 2 * c + core
        return pltpu.make_async_remote_copy(
            src_ref=a_rows(s, c, core), dst_ref=a_hbm.at[me * per + s],
            send_sem=a_send.at[s, tgt], recv_sem=a_recv.at[s, me],
            device_id={'sp': tgt}, device_id_type=pl.DeviceIdType.MESH)

    def a_local(s):
        return pltpu.make_async_copy(a_rows(s, my_chip, my_core), a_hbm.at[me * per + s], aloc_sem.at[s])

    def out_chunk(s, c):
        row0 = pl.multiple_of(s * seq + c * ch, ch)

        for j in range(tiles):
            cols = pl.ds(j * TN, TN)
            q_buf[pl.ds(row0, ch), cols] = jnp.dot(
                o_buf[...], wo[:, cols], preferred_element_type=F32).astype(BF16)

    def phase(s, carry):
        start = jnp.where(s == 0, -n_own, jnp.where(s < per, 0, chips - 1))

        @pl.when(s == 0)
        def _():
            wait_x(0, sib)
            half_copy(xr_hbm.at[0, sib], 0, 1 - my_core).start()

        @pl.when(jnp.logical_and(s > 0, s < per))
        def _():
            load_other(s, lax.rem(my_chip + offset_of(0), chips), 0)

        def chunk(i, carry):
            own = i < 0
            sq = jnp.where(own, i + n_own, s)
            c = jnp.where(own, my_chip, lax.rem(my_chip + offset_of(i), chips))
            slot = lax.rem(i - start, 2)

            def prefetch():
                nxt = i + 1

                @pl.when(nxt < 0)
                def _():
                    load_own(nxt + n_own, 1 - slot)

                @pl.when(jnp.logical_and(nxt >= 0, nxt < chips - 1))
                def _():
                    load_other(s, lax.rem(my_chip + offset_of(nxt), chips), 1 - slot)

            @pl.when(jnp.logical_and(s == 0, i == -n_own))
            def _():
                for d in range(1, n):
                    wait_pos(lax.rem(me + d, n))
            qkv_chunk(sq, c, slot, jnp.logical_and(s == 0, i == -n_own), prefetch)
            return carry
        lax.fori_loop(start, chips - 1, chunk, 0)

        @pl.when(s == 0)
        def _():
            weight_copy(3).wait()

        def out_step(i, carry):
            up = lax.rem(my_chip + 1, chips)
            down = lax.rem(my_chip + chips - 1, chips)
            own = s == per
            sq = jnp.where(own, i, s)
            c = lax.rem(my_chip + offset_of(i), chips)
            c = jnp.where(i == 0, jnp.minimum(up, down), jnp.where(i == 1, jnp.maximum(up, down), c))
            c = jnp.where(own, my_chip, c)
            for blk_i in range(chips):
                @pl.when(c == blk_i)
                def _():
                    attend(sq, blk_i)
            out_chunk(sq, c)
            for core in range(2):
                mine = jnp.logical_and(c == my_chip, core == my_core)

                @pl.when(mine)
                def _():
                    a_local(sq).start()

                @pl.when(jnp.logical_not(mine))
                def _():
                    a_copy(sq, c, core).start()
            return carry
        lax.fori_loop(0, jnp.where(s < per, chips - 1, per), out_step, 0)
        return carry

    lax.fori_loop(0, per + 1, phase, 0)

    home = [(0, 1)] + [(dc, fl) for fl in (0, 1) for dc in (chips - 1, 1)] + partners[5:]

    def a_arrival(s, src):
        return pltpu.make_async_remote_copy(
            src_ref=q_buf.at[pl.ds(0, blk)], dst_ref=a_hbm.at[src * per + s],
            send_sem=a_send.at[s, src], recv_sem=a_recv.at[s, src],
            device_id={'sp': sib}, device_id_type=pl.DeviceIdType.MESH)

    def source(t):
        s = t // n
        r = lax.rem(t, n)
        src = me
        for k, (dc, fl) in enumerate(home):
            src = jnp.where(r == k + 1, partner(dc, fl), src)
        return s, src

    def fin_loads(t, slot):
        s, src = source(t)
        return (pltpu.make_async_copy(a_hbm.at[src * per + s], x_buf.at[slot, pl.ds(0, blk)], ld_sem.at[slot, 0]),
                pltpu.make_async_copy(x_hbm.at[src * per + s], x_buf.at[slot, pl.ds(blk, blk)], ld_sem.at[slot, 1]))

    def fin_store(t, slot):
        s, src = source(t)
        return pltpu.make_async_copy(x_buf.at[slot, pl.ds(0, blk)], y_hbm.at[src * per + s], out_sem.at[slot])

    def fin_fetch(t, slot):
        s, src = source(t)

        @pl.when(src == me)
        def _():
            a_local(s).wait()

        @pl.when(src != me)
        def _():
            a_arrival(s, src).wait_recv()
        for cp in fin_loads(t, slot):
            cp.start()

    steps = per * n
    fin_fetch(0, 0)

    def fin_step(t, carry):
        slot = lax.rem(t, 2)

        @pl.when(t >= 1)
        def _():
            fin_store(t - 1, 1 - slot).wait()

        @pl.when(t + 1 < steps)
        def _():
            fin_fetch(t + 1, 1 - slot)
        for cp in fin_loads(t, slot):
            cp.wait()
        acc = jnp.zeros((blk, HEAD_DIM), F32)
        for h in range(heads):
            v = x_buf[slot, 0:blk, h * HEAD_DIM:(h + 1) * HEAD_DIM].astype(F32)
            acc = acc + v * v
        r = lax.rsqrt(jnp.sum(acc, axis=1, keepdims=True) * (1.0 / width) + NORM_EPS)
        for h in range(heads):
            cols = slice(h * HEAD_DIM, (h + 1) * HEAD_DIM)
            v = x_buf[slot, 0:blk, cols].astype(F32) * r * g_tab[2:3, cols]
            x_buf[slot, 0:blk, cols] = (x_buf[slot, blk:2 * blk, cols].astype(F32) + v).astype(BF16)
        fin_store(t, slot).start()
        return carry
    lax.fori_loop(0, steps, fin_step, 0)
    fin_store(steps - 1, (steps - 1) % 2).wait()

    for s in range(per):
        for pi in range(n - 1):
            x_copy(pi, s).wait_send()
            a_arrival(s, partner(*partners[pi])).wait_send()
    for pi in range(n - 1):
        pos_copy(pi).wait_send()


def exchange_attention(n, x_loc, pos_loc, w_query, w_key, w_value, w_out, gain_q, gain_k, gain_out):
    batch, blk, width = x_loc.shape
    per = batch // n
    seq = n * blk
    freq = (1.0 / (np.float32(ROPE_THETA) ** (np.arange(0, HEAD_DIM, 2, dtype=np.float32) / np.float32(HEAD_DIM)))).astype(np.float32)
    freq = jnp.asarray(np.concatenate([freq, freq])[None, :])
    hbm = pl.BlockSpec(memory_space=pl.ANY)
    vmem = pl.BlockSpec(memory_space=pltpu.VMEM)
    dma = pltpu.SemaphoreType.DMA
    wbuf = pltpu.VMEM((width, width), BF16)
    sbuf = pltpu.VMEM((per * seq, width), BF16)
    tab = pltpu.VMEM((2 * blk, HEAD_DIM), F32)
    return pl.pallas_call(
        functools.partial(kernel, n, per, blk, width),
        out_shape=(jax.ShapeDtypeStruct((per, n, blk, width), BF16), jax.ShapeDtypeStruct((batch, blk, width), BF16),
                   jax.ShapeDtypeStruct((batch, blk, width), BF16)),
        in_specs=[hbm] * 6 + [vmem] * 4,
        out_specs=(hbm, hbm, hbm),
        scratch_shapes=[
            wbuf, wbuf, wbuf, wbuf, sbuf, sbuf, pltpu.VMEM((per, width, seq), BF16),
            pltpu.VMEM((2, 2 * blk, width), BF16),
            pltpu.VMEM((n, batch, blk), jnp.int32),
            tab, tab, tab, tab,
            pltpu.VMEM((2, seq, 2 * blk), F32), pltpu.VMEM((2 * blk, width), BF16), pltpu.VMEM((3, width), F32),
            dma((4,)), dma, dma((2, 2)), dma((per,)), dma((2,)),
            dma((per, n)), dma((per, n)), dma((n,)), dma((n,)), dma((per, n)), dma((per, n)),
        ],
        compiler_params=pltpu.CompilerParams(
            collective_id=0, has_side_effects=True, vmem_limit_bytes=67043328),
        name='exchange_attention',
    )(x_loc, pos_loc, w_query, w_key, w_value, w_out, gain_q, gain_k, gain_out, freq)[2]


def solution(mesh):
    n = mesh.shape['sp']

    def local_block(x_loc, pos_loc, w_query, w_key, w_value, w_out, gain_q, gain_k, gain_out):
        return exchange_attention(n, x_loc, pos_loc, w_query, w_key, w_value, w_out, gain_q, gain_k, gain_out)

    tok_spec = P('dp', 'sp', None)
    return jax.shard_map(local_block, mesh=mesh, in_specs=(tok_spec, P('dp', 'sp'), P(), P(), P(), P(), P(), P(), P()), out_specs=tok_spec, check_vma=False)
```
